32 devices in a mesh: tm: 8 (over z, x), mp: 4 (over y, core).
Axes of the slice: x: 2, y: 2, z: 4, core: 2. Of those that a mesh axis runs over, the one named last changes fastest.
Arguments:
- features: bfloat16 [256, 2048], P('tm'), may hold values from -6 to 6
- w_in: bfloat16 [2048, 4096], P(None, 'mp'), may hold values from -0.125 to 0.125
- b_in: float32 [4096], P('mp'), may hold values from -5 to 5
- output_weight: bfloat16 [4096, 256], P('mp'), may hold values from -0.09375 to 0.09375
- final_offset_entries: float32 [256], replicated, may hold values from -3 to 3
- transition: float32 [256, 256], replicated, may hold values from -1 to 1
- gains: float32 [256, 256], P('tm'), may hold values from 0 to 1
- smooth_gains: float32 [256, 256], P('tm'), may hold values from 0 to 1
Outputs:
- filtered: float32 [256, 256], P(('tm', 'mp'))
- smoothed: float32 [256, 256], P(('tm', 'mp'))
The draws below stay inside these ranges and needn't reach their ends.
All inputs are finite; a program needn't handle non-finite values.
Results may differ from the reference program's by a relative error of at most 0.0021.
Values sent between devices are 32-bit elements; how exact they have to be, the bound alone decides.
A program may use at most 128 MiB of HBM per device.

```python
import math
import jax
import jax.numpy as jnp
from jax import lax

GRID = 256
HID_UNITS = 4096
FR_DEV = 32
FEATURES = 2048
TRACK_SNAPSHOTS = 256


def retention_field(key):
    sampler_seeds = jax.random.split(key, 5)
    low = math.log(0.1 / TRACK_SNAPSHOTS)
    high = math.log(1.0 / 30.0)
    channel = jnp.exp(jax.random.uniform(sampler_seeds[0], (1, GRID), jnp.float32, low, high))
    blocks = jnp.exp(jax.random.uniform(sampler_seeds[1], (TRACK_SNAPSHOTS // FR_DEV, 1), jnp.float32, -0.7, 0.7))
    blocks = jnp.repeat(blocks, FR_DEV, axis=0)
    rough = jax.random.uniform(sampler_seeds[2], (TRACK_SNAPSHOTS, GRID), jnp.float32, 0.5, 1.5)
    forgetting_factor = channel * blocks * rough
    cluster_extent = jax.random.bernoulli(sampler_seeds[3], 4.0 / TRACK_SNAPSHOTS, (TRACK_SNAPSHOTS, 1)).astype(jnp.float32)
    doubling_height = jax.random.uniform(sampler_seeds[4], (1, GRID), jnp.float32, 0.2, 0.5)
    return jnp.exp(-forgetting_factor) * (1.0 - cluster_extent * doubling_height)


def draw_transition(key, part):
    raw = jax.random.normal(jax.random.fold_in(key, 5), (GRID, GRID), jnp.float32) * (0.6 / math.sqrt(GRID))
    skew = raw - raw.T
    eye = jnp.eye(GRID, dtype=jnp.float32)
    return jnp.linalg.solve(eye - skew, eye + skew).astype(jnp.float32)


def draw_gains(key, part):
    return (1.0 - retention_field(jax.random.fold_in(key, 11))).astype(jnp.float32)


def draw_smooth_gains(key, part):
    return retention_field(jax.random.fold_in(key, 23)).astype(jnp.float32)


def block_levels(key, extent, cuts, low, high):
    level = 1.0
    for dim, parts in cuts:
        draws = jax.random.uniform(jax.random.fold_in(jax.random.fold_in(key, 6), dim), (parts,), jnp.float32, low / len(cuts), high / len(cuts))
        level = level * jnp.repeat(jnp.exp(draws), extent[dim] // parts).reshape((-1,) + (1,) * (len(extent) - 1 - dim))
    return level


def scatter_about(own_key, extent, deviation, limit, cuts=(), kind=jnp.bfloat16):
    result = jax.random.normal(own_key, extent, jnp.float32) * deviation
    if len(cuts) > 0:
        result = block_levels(own_key, extent, cuts, -0.22, 0.18) * result
    return jnp.clip(result, min=-limit, max=limit).astype(kind)


def setup_inputs(seed: int = 0) -> dict:
    key_list = jax.random.split(jax.random.key(seed), 9)
    return {
        "features": scatter_about(key_list[0], (TRACK_SNAPSHOTS, FEATURES), 1.0, 6.0, ((0, 8),)),
        "w_in": scatter_about(key_list[1], (FEATURES, HID_UNITS), FEATURES ** -0.5, 0.125, ((1, 4),)),
        "b_in": scatter_about(key_list[2], (HID_UNITS,), 1.0, 5.0, ((0, 4),), jnp.float32),
        "output_weight": scatter_about(key_list[3], (HID_UNITS, GRID), HID_UNITS ** -0.5, 0.09375, ((0, 4),)),
        "final_offset_entries": scatter_about(key_list[4], (GRID,), 0.5, 3.0, (), jnp.float32),
        "transition": draw_transition(jax.random.fold_in(key_list[8], 71), 0),
        "gains": draw_gains(jax.random.fold_in(key_list[8], 71), 0),
        "smooth_gains": draw_smooth_gains(jax.random.fold_in(key_list[8], 71), 0),
    }


def reference(features, w_in, b_in, output_weight, final_offset_entries, transition, gains, smooth_gains):
    pre = jnp.dot(features.astype(jnp.float32), w_in.astype(jnp.float32), preferred_element_type=jnp.float32) + b_in
    hidden_layer = jax.nn.gelu(pre, approximate=True).astype(jnp.bfloat16)
    measured_values = jnp.dot(hidden_layer.astype(jnp.float32), output_weight.astype(jnp.float32), preferred_element_type=jnp.float32) + final_offset_entries

    def forward_pass(state, current_row):
        gain_vector, measurement_row = current_row
        moved_state = jnp.dot(transition, state, precision=lax.Precision.HIGHEST)
        fresh_value = (1.0 - gain_vector) * moved_state + gain_vector * measurement_row
        return (fresh_value, fresh_value)
    start_index = jnp.zeros((GRID,), jnp.float32)
    unused_item, filtered = lax.scan(forward_pass, start_index, (gains, measured_values))
    predicted = jnp.dot(filtered, transition.T, precision=lax.Precision.HIGHEST)
    weight = smooth_gains.at[-1].set(0.0)

    def backward(state, current_row):
        weight_row, filt_row, pred_row = current_row
        fresh_value = filt_row + weight_row * (state - pred_row)
        return (fresh_value, fresh_value)
    unused_item, smoothed = lax.scan(backward, start_index, (weight, filtered, predicted), reverse=True)
    return (filtered, smoothed)
```

```python
import functools

import jax
import jax.numpy as jnp
from jax import lax
from jax.experimental import pallas as pl
from jax.experimental.pallas import tpu as pltpu
from jax.sharding import PartitionSpec as P

MESH = pl.DeviceIdType.MESH
F32 = jnp.float32
BF16 = jnp.bfloat16


def split(value):
    high = value.astype(BF16).astype(F32)
    return high, value - high


def store_split(target, value):
    width = value.shape[1]
    high, rest = split(value)
    target[:, :width] = high.astype(BF16)
    target[:, width:] = rest.astype(BF16)


def times(rows, pair):
    count, width = rows.shape
    both = jnp.concatenate(split(rows), 0).astype(BF16)
    out = jnp.dot(both, pair[...], preferred_element_type=F32)
    return out[:count, :width] + out[count:, :width] + out[:count, width:]


def kernel(
    tm, mp, chunks,
    feat_h, w_in_h, b_h, w2_h, off_h, trans_h, gains_h, sg_h,
    filt_o, smooth_o,
    feat, w_in, b_v, w2, off, trans, gains, sg,
    at, at_pair, m_pair, phi_pair, part, meas, snap, m_all, phi_all, vel, x_in, x_out, x_own,
    f8, u8, e8, comp, comps,
    in_sem, part_ss, part_rs, m_ss, m_rs, phi_ss, phi_rs, chain_ss, chain_rs, back_ss, back_rs,
):
    c, k = lax.axis_index("tm"), lax.axis_index("mp")
    place = c * mp + k
    total = tm * mp
    frames, grid = gains.shape
    share = frames // mp
    quarter = grid // mp
    depth = feat.shape[1] // chunks

    def fetch(source, target, slot):
        copy = pltpu.make_async_copy(source, target, in_sem.at[slot])
        copy.start()
        return copy

    get_trans = fetch(trans_h, trans, 0)
    get_gains = fetch(gains_h, gains, 1)
    get_feat = fetch(feat_h, feat, 2)
    get_w = [
        fetch(w_in_h.at[pl.ds(r * depth, depth), :], w_in.at[pl.ds(r * depth, depth), :], 8 + r)
        for r in range(chunks)
    ]
    get_b = fetch(b_h, b_v, 3)
    get_w2 = fetch(w2_h, w2, 4)
    get_off = fetch(off_h, off, 5)
    get_sg = fetch(sg_h, sg, 6)

    barrier = pltpu.get_barrier_semaphore()

    def greet(step, carry):
        other = lax.rem(place + step, total)
        pl.semaphore_signal(
            barrier, inc=1, device_id={"tm": other // mp, "mp": lax.rem(other, mp)},
            device_id_type=MESH,
        )
        return carry

    lax.fori_loop(1, total, greet, 0)

    get_trans.wait()
    get_gains.wait()
    at[...] = jnp.transpose(trans[...])
    store_split(at_pair, at[...])
    rows = at[pl.ds(pl.multiple_of(k * quarter, quarter), quarter), :] * (1.0 - gains[0:1, :])
    get_feat.wait()
    pre = jnp.zeros((frames, w_in.shape[1]), F32)
    pace = frames // chunks
    for r in range(chunks):
        get_w[r].wait()
        pre += jnp.dot(
            feat[:, r * depth : (r + 1) * depth], w_in[r * depth : (r + 1) * depth, :],
            preferred_element_type=F32,
        )
        for t in range(r * pace, (r + 1) * pace):
            if t > 0:
                rows = times(rows, at_pair) * (1.0 - gains[t : t + 1, :])
            if (t + 1) % share == 0:
                snap[(t + 1) // share - 1] = rows
    get_b.wait()
    get_w2.wait()
    hidden = jax.nn.gelu(pre + b_v[...], approximate=True).astype(BF16)
    part[k] = jnp.dot(hidden, w2[...], preferred_element_type=F32)

    pl.semaphore_wait(barrier, total - 1)

    def to_peer(step, source, target, send, recv):
        peer = lax.rem(k + step, mp)
        return pltpu.make_async_remote_copy(
            source, target, send.at[step], recv.at[step],
            device_id={"tm": c, "mp": peer}, device_id_type=MESH,
        )

    def phi_copy(step):
        peer = lax.rem(k + step, mp)
        return pltpu.make_async_remote_copy(
            snap.at[lax.rem(peer + mp - 1, mp)], phi_all.at[k], phi_ss.at[step], phi_rs.at[step],
            device_id={"tm": c, "mp": peer}, device_id_type=MESH,
        )

    part_copies = [to_peer(s, part.at[k], part.at[k], part_ss, part_rs) for s in range(1, mp)]
    m_copies = [to_peer(s, snap.at[mp - 1], m_all.at[k], m_ss, m_rs) for s in range(1, mp)]
    phi_copies = [phi_copy(s) for s in range(1, mp)]
    for copy in part_copies:
        copy.start()
    for copy in m_copies:
        copy.start()
    for copy in phi_copies:
        copy.start()
    m_all[k] = snap[mp - 1]
    phi_all[k] = snap[lax.rem(k + mp - 1, mp)]
    get_off.wait()
    get_sg.wait()
    for copy in part_copies:
        copy.wait_recv()
    measured = off[...]
    for peer in range(mp):
        measured = measured + part[peer]
    meas[...] = gains[...] * measured

    def frame(t, state):
        keep = 1.0 - gains[pl.ds(t, 1), :]
        return times(state, at_pair) * keep + meas[pl.ds(t, 1), :]

    def pass_frames(block, state):
        for j in range(share):
            t = block * share + j
            state = frame(t, state)
            vel[pl.ds(t, 1), :] = state[0:1]
        return state

    vel_end = lax.fori_loop(0, mp, pass_frames, jnp.zeros((8, grid), F32))
    for copy in m_copies:
        copy.wait_recv()
    store_split(m_pair, m_all[...].reshape(grid, grid))
    for copy in phi_copies:
        copy.wait_recv()
    store_split(phi_pair, phi_all[...].reshape(grid, grid))

    chain = pltpu.make_async_remote_copy(
        x_out, x_in, chain_ss, chain_rs,
        device_id={"tm": lax.rem(c + 1, tm), "mp": k}, device_id_type=MESH,
    )

    @pl.when(c == 0)
    def _():
        x_in[...] = jnp.zeros_like(x_in)
        x_out[...] = vel_end

    @pl.when(c > 0)
    def _():
        chain.wait_recv()
        x_out[...] = times(x_in[...], m_pair) + vel_end

    @pl.when(c < tm - 1)
    def _():
        chain.start()

    @pl.when(k == 0)
    def _():
        x_own[...] = x_in[...]

    @pl.when(k > 0)
    def _():
        x_own[...] = times(x_in[...], phi_pair) + vel[pl.ds(k * share - 1, 1), :]

    state = x_own[...]
    for j in range(share):
        state = frame(k * share + j, state)
        f8[j : j + 1, :] = state[0:1]
    filtered = f8[...]
    filt_o[...] = filtered
    last = jnp.where(place == total - 1, 0.0, 1.0).astype(F32)
    row = lax.broadcasted_iota(jnp.int32, (share, grid), 0)
    weight = sg[pl.ds(pl.multiple_of(k * share, share), share), :]
    weight = jnp.where(row == share - 1, weight * last, weight)
    e8[...] = weight
    u8[...] = filtered - weight * times(filtered, at_pair)
    slope = jnp.ones((1, grid), F32)
    value = jnp.zeros((1, grid), F32)
    for j in range(share - 1, -1, -1):
        slope = slope * e8[j : j + 1, :]
        value = u8[j : j + 1, :] + e8[j : j + 1, :] * value
    comp[0:1, :] = slope
    comp[1:2, :] = value

    def back_copy(other):
        return pltpu.make_async_remote_copy(
            comp, comps.at[place], back_ss.at[other], back_rs.at[place],
            device_id={"tm": other // mp, "mp": lax.rem(other, mp)}, device_id_type=MESH,
        )

    def send_back(step, carry):
        back_copy(place - 1 - step).start()
        return carry

    lax.fori_loop(0, place, send_back, 0)

    def gather_back(step, later):
        source = total - 1 - step
        pltpu.make_async_remote_copy(
            comp, comps.at[source], back_ss.at[source], back_rs.at[source],
            device_id={"tm": source // mp, "mp": lax.rem(source, mp)}, device_id_type=MESH,
        ).wait_recv()
        both = comps[source]
        return both[0:1] * later + both[1:2]

    later = lax.fori_loop(0, total - 1 - place, gather_back, jnp.zeros((1, grid), F32))
    for j in range(share - 1, -1, -1):
        later = u8[j : j + 1, :] + e8[j : j + 1, :] * later
        smooth_o[j : j + 1, :] = later

    def end_back(other, carry):
        back_copy(other).wait_send()
        return carry

    lax.fori_loop(0, place, end_back, 0)
    for copy in part_copies + m_copies + phi_copies:
        copy.wait_send()

    @pl.when(c < tm - 1)
    def _():
        chain.wait_send()


def on_device(features, w_in, b_in, output_weight, offset, transition, gains, smooth_gains):
    tm, mp = lax.axis_size("tm"), lax.axis_size("mp")
    frames, lags = features.shape
    units = w_in.shape[1]
    grid = transition.shape[0]
    share = frames // mp
    quarter = grid // mp
    chunks = 8
    args = (
        features, w_in, b_in.reshape(1, units), output_weight, offset.reshape(1, grid),
        transition, gains, smooth_gains,
    )
    dma = pltpu.SemaphoreType.DMA
    out = jax.ShapeDtypeStruct((share, grid), F32)
    return pl.pallas_call(
        functools.partial(kernel, tm, mp, chunks),
        out_shape=(out, out),
        in_specs=[pl.BlockSpec(memory_space=pl.ANY)] * len(args),
        out_specs=(pl.BlockSpec(memory_space=pltpu.VMEM),) * 2,
        scratch_shapes=[pltpu.VMEM(a.shape, a.dtype) for a in args]
        + [
            pltpu.VMEM((grid, grid), F32),
            pltpu.VMEM((grid, 2 * grid), BF16),
            pltpu.VMEM((grid, 2 * grid), BF16),
            pltpu.VMEM((grid, 2 * grid), BF16),
            pltpu.VMEM((mp, frames, grid), F32),
            pltpu.VMEM((frames, grid), F32),
            pltpu.VMEM((mp, quarter, grid), F32),
            pltpu.VMEM((mp, quarter, grid), F32),
            pltpu.VMEM((mp, quarter, grid), F32),
            pltpu.VMEM((frames, grid), F32),
            pltpu.VMEM((8, grid), F32),
            pltpu.VMEM((8, grid), F32),
            pltpu.VMEM((8, grid), F32),
            pltpu.VMEM((share, grid), F32),
            pltpu.VMEM((share, grid), F32),
            pltpu.VMEM((share, grid), F32),
            pltpu.VMEM((2, grid), F32),
            pltpu.VMEM((tm * mp, 2, grid), F32),
            dma((8 + chunks,)),
            dma((mp,)), dma((mp,)), dma((mp,)), dma((mp,)), dma((mp,)), dma((mp,)),
            dma(()), dma(()),
            dma((tm * mp,)), dma((tm * mp,)),
        ],
        compiler_params=pltpu.CompilerParams(collective_id=0, has_side_effects=True),
        name="track",
    )(*args)


def solution(mesh):
    placed = (
        P("tm", None),
        P(None, "mp"),
        P("mp"),
        P("mp", None),
        P(),
        P(),
        P("tm", None),
        P("tm", None),
    )
    return jax.shard_map(
        on_device,
        mesh=mesh,
        in_specs=placed,
        out_specs=(P(("tm", "mp"), None), P(("tm", "mp"), None)),
        check_vma=False,
    )
```

```python
import functools
import math

import jax
import jax.numpy as jnp
from jax import lax
from jax.experimental import pallas as pl
from jax.experimental.pallas import tpu as pltpu
from jax.sharding import PartitionSpec as P

MESH = pl.DeviceIdType.MESH
F32 = jnp.float32
BF16 = jnp.bfloat16
GROUP = 4


def split(value):
    high = value.astype(BF16).astype(F32)
    return high, value - high


def store_split(target, value):
    width = value.shape[1]
    high, rest = split(value)
    target[:, :width] = high.astype(BF16)
    target[:, width:] = rest.astype(BF16)


def times(rows, pair):
    count, width = rows.shape
    both = jnp.concatenate(split(rows), 0).astype(BF16)
    out = jnp.dot(both, pair[...], preferred_element_type=F32)
    return out[:count, :width] + out[count:, :width] + out[:count, width:]


def kernel(
    tm, mp, chunks, group,
    feat_h, w_in_h, b_h, w2_h, off_h, trans_h, gains_h, sg_h,
    packed,
    feat, w_in, b_v, w2, off, trans, gains, sg,
    at, at_pair, m_pair, phi_pair, part, meas, snap, m_all, phi_all, vel, v_all, x_in, x_out, x_own,
    f8, u8, e8, comp, comps,
    in_sem, part_ss, part_rs, r1_ss, r1_rs, r2_ss, r2_rs, r3_ss, r3_rs, r4_ss, r4_rs,
    phi_ss, phi_rs, v_ss, v_rs, chain_ss, chain_rs, back_ss, back_rs,
):
    c, k = lax.axis_index("tm"), lax.axis_index("mp")
    place = c * mp + k
    total = tm * mp
    here, set_c = lax.rem(c, group), c // group
    sets = tm // group
    across = lax.rem(k + mp // 2, mp)
    beside = k + 1 - 2 * lax.rem(k, 2)
    frames, grid = gains.shape
    share = frames // mp
    quarter = grid // mp
    depth = feat.shape[1] // chunks

    def fetch(source, target, slot):
        copy = pltpu.make_async_copy(source, target, in_sem.at[slot])
        copy.start()
        return copy

    get_trans = fetch(trans_h, trans, 0)
    get_gains = fetch(gains_h, gains, 1)
    get_feat = fetch(feat_h, feat, 2)
    get_w = [
        fetch(w_in_h.at[pl.ds(r * depth, depth), :], w_in.at[pl.ds(r * depth, depth), :], 8 + r)
        for r in range(chunks)
    ]
    get_b = fetch(b_h, b_v, 3)
    get_w2 = fetch(w2_h, w2, 4)
    get_off = fetch(off_h, off, 5)
    get_sg = fetch(sg_h, sg, 6)

    barrier = pltpu.get_barrier_semaphore()

    def greet(step, carry):
        other = lax.rem(place + step, total)
        pl.semaphore_signal(
            barrier, inc=1, device_id={"tm": other // mp, "mp": lax.rem(other, mp)},
            device_id_type=MESH,
        )
        return carry

    lax.fori_loop(1, total, greet, 0)

    get_trans.wait()
    get_gains.wait()
    at[...] = jnp.transpose(trans[...])
    store_split(at_pair, at[...])
    rows = at[pl.ds(pl.multiple_of(k * quarter, quarter), quarter), :] * (1.0 - gains[0:1, :])
    get_feat.wait()
    pre = jnp.zeros((frames, w_in.shape[1]), F32)
    def advance(rows, first, end):
        for t in range(first, end):
            if t > 0:
                rows = times(rows, at_pair) * (1.0 - gains[t : t + 1, :])
            if (t + 1) % share == 0:
                snap[(t + 1) // share - 1] = rows
        return rows

    pace = frames // chunks // 2
    for r in range(chunks):
        get_w[r].wait()
        pre += jnp.dot(
            feat[:, r * depth : (r + 1) * depth], w_in[r * depth : (r + 1) * depth, :],
            preferred_element_type=F32,
        )
        rows = advance(rows, r * pace, (r + 1) * pace)
    get_b.wait()
    get_w2.wait()
    hidden = jax.nn.gelu(pre + b_v[...], approximate=True).astype(BF16)
    part[k] = jnp.dot(hidden, w2[...], preferred_element_type=F32)

    pl.semaphore_wait(barrier, total - 1)

    def remote(source, target, send, recv, c_to, k_to):
        return pltpu.make_async_remote_copy(
            source, target, send, recv, device_id={"tm": c_to, "mp": k_to}, device_id_type=MESH
        )

    def phi_copy(step):
        peer = lax.rem(k + step, mp)
        return remote(
            snap.at[lax.rem(peer + mp - 1, mp)], phi_all.at[k], phi_ss.at[step], phi_rs.at[step],
            c, peer,
        )

    def in_set(step, source, target, send, recv):
        peer = set_c * group + lax.rem(here + step, group)
        return remote(source, target, send.at[step], recv.at[step], peer, k)

    part_copies = [
        remote(part.at[k], part.at[k], part_ss.at[s], part_rs.at[s], c, lax.rem(k + s, mp))
        for s in range(1, mp)
    ]
    for copy in part_copies:
        copy.start()
    rows = advance(rows, pace * chunks, frames)

    own = snap.at[mp - 1]
    come = [lax.rem(here + group - s, group) for s in range(group)]
    r1 = [in_set(s, own, m_all.at[here, k], r1_ss, r1_rs) for s in range(1, group)]
    r2, r3, r4 = [], [], []
    for s in range(group):
        j = come[s]
        mine = own if s == 0 else m_all.at[j, k]
        r2.append(remote(mine, m_all.at[j, k], r2_ss.at[s], r2_rs.at[s], c, across))
        r3.append(remote(mine, m_all.at[j, k], r3_ss.at[s], r3_rs.at[s], c, beside))
        r4.append(
            remote(m_all.at[j, across], m_all.at[j, across], r4_ss.at[s], r4_rs.at[s], c, beside)
        )
    phi_copies = [phi_copy(s) for s in range(1, mp)]
    for copy in r1 + r2[:1] + r3[:1]:
        copy.start()
    m_all[here, k] = snap[mp - 1]
    phi_all[k] = snap[lax.rem(k + mp - 1, mp)]
    get_off.wait()
    get_sg.wait()
    for copy in part_copies:
        copy.wait_recv()
    measured = off[...]
    for peer in range(mp):
        measured = measured + part[peer]
    meas[...] = gains[...] * measured

    def frame(t, state):
        keep = 1.0 - gains[pl.ds(t, 1), :]
        return times(state, at_pair) * keep + meas[pl.ds(t, 1), :]

    def pass_frames(block, state):
        for j in range(share):
            t = block * share + j
            state = frame(t, state)
            vel[pl.ds(t, 1), :] = state[0:1]
        return state

    early = mp // 2
    vel_end = lax.fori_loop(0, early, pass_frames, jnp.zeros((8, grid), F32))
    for s in range(1, group):
        r1[s - 1].wait_recv()
        r2[s].start()
        r3[s].start()
    for copy in phi_copies:
        copy.start()
    vel_end = lax.fori_loop(early, mp, pass_frames, vel_end)
    v_all[here] = vel_end
    v_copies = [in_set(s, v_all.at[here], v_all.at[here], v_ss, v_rs) for s in range(1, group)]
    for copy in v_copies:
        copy.start()
    for s in range(group):
        r2[s].wait_recv()
        r4[s].start()
    for s in range(group):
        r3[s].wait_recv()
        r4[s].wait_recv()
        store_split(m_pair.at[come[s]], m_all[come[s]].reshape(grid, grid))
    for copy in v_copies:
        copy.wait_recv()

    chain = remote(x_out, x_in, chain_ss, chain_rs, lax.rem(c + group, tm), k)

    @pl.when(set_c == 0)
    def _():
        x_in[...] = jnp.zeros_like(x_in)

    @pl.when(set_c > 0)
    def _():
        chain.wait_recv()

    def whole_block(j, state):
        return times(state, m_pair.at[j]) + v_all[j]

    state = lax.fori_loop(0, here, whole_block, x_in[...])

    @pl.when(set_c < sets - 1)
    def _():
        x_out[...] = lax.fori_loop(here, group, whole_block, state)
        chain.start()

    x_in[...] = state
    for copy in phi_copies:
        copy.wait_recv()
    store_split(phi_pair, phi_all[...].reshape(grid, grid))

    @pl.when(k == 0)
    def _():
        x_own[...] = x_in[...]

    @pl.when(k > 0)
    def _():
        x_own[...] = times(x_in[...], phi_pair) + vel[pl.ds(k * share - 1, 1), :]

    state = x_own[...]
    for j in range(share):
        state = frame(k * share + j, state)
        f8[j : j + 1, :] = state[0:1]
    filtered = f8[...]
    packed[:share, :] = filtered
    last = jnp.where(place == total - 1, 0.0, 1.0).astype(F32)
    row = lax.broadcasted_iota(jnp.int32, (share, grid), 0)
    weight = sg[pl.ds(pl.multiple_of(k * share, share), share), :]
    weight = jnp.where(row == share - 1, weight * last, weight)
    e8[...] = weight
    u8[...] = filtered - weight * times(filtered, at_pair)
    packed[share : 2 * share, :] = u8[...]
    packed[2 * share : 3 * share, :] = weight
    slope = jnp.ones((1, grid), F32)
    value = jnp.zeros((1, grid), F32)
    for j in range(share - 1, -1, -1):
        slope = slope * e8[j : j + 1, :]
        value = u8[j : j + 1, :] + e8[j : j + 1, :] * value
    comp[0:1, :] = slope
    comp[1:2, :] = value

    def back_copy(other):
        return pltpu.make_async_remote_copy(
            comp, comps.at[place], back_ss.at[other], back_rs.at[place],
            device_id={"tm": other // mp, "mp": lax.rem(other, mp)}, device_id_type=MESH,
        )

    def send_back(step, carry):
        back_copy(place - 1 - step).start()
        return carry

    lax.fori_loop(0, place, send_back, 0)

    def gather_back(step, later):
        source = total - 1 - step
        pltpu.make_async_remote_copy(
            comp, comps.at[source], back_ss.at[source], back_rs.at[source],
            device_id={"tm": source // mp, "mp": lax.rem(source, mp)}, device_id_type=MESH,
        ).wait_recv()
        both = comps[source]
        return both[0:1] * later + both[1:2]

    later = lax.fori_loop(0, total - 1 - place, gather_back, jnp.zeros((1, grid), F32))
    packed[3 * share :, :] = jnp.broadcast_to(later, (8, grid))

    def end_back(other, carry):
        back_copy(other).wait_send()
        return carry

    lax.fori_loop(0, place, end_back, 0)
    for copy in part_copies + r1 + r2 + r3 + r4 + v_copies + phi_copies:
        copy.wait_send()

    @pl.when(set_c < sets - 1)
    def _():
        chain.wait_send()


def finish(share, packed, filt_o, smooth_o):
    filt_o[...] = packed[:share, :]
    later = packed[3 * share : 3 * share + 1, :]
    for j in range(share - 1, -1, -1):
        fresh, weight = share + j, 2 * share + j
        later = packed[fresh : fresh + 1, :] + packed[weight : weight + 1, :] * later
        smooth_o[j : j + 1, :] = later


def on_device(features, w_in, b_in, output_weight, offset, transition, gains, smooth_gains):
    tm, mp = lax.axis_size("tm"), lax.axis_size("mp")
    frames, lags = features.shape
    units = w_in.shape[1]
    grid = transition.shape[0]
    share = frames // mp
    quarter = grid // mp
    chunks = 8
    group = math.gcd(tm, GROUP)
    args = (
        features, w_in, b_in.reshape(1, units), output_weight, offset.reshape(1, grid),
        transition, gains, smooth_gains,
    )
    dma = pltpu.SemaphoreType.DMA
    out = jax.ShapeDtypeStruct((share, grid), F32)
    packed = pl.pallas_call(
        functools.partial(kernel, tm, mp, chunks, group),
        out_shape=jax.ShapeDtypeStruct((3 * share + 8, grid), F32),
        in_specs=[pl.BlockSpec(memory_space=pl.ANY)] * len(args),
        out_specs=pl.BlockSpec(memory_space=pltpu.VMEM),
        scratch_shapes=[pltpu.VMEM(a.shape, a.dtype) for a in args]
        + [
            pltpu.VMEM((grid, grid), F32),
            pltpu.VMEM((grid, 2 * grid), BF16),
            pltpu.VMEM((group, grid, 2 * grid), BF16),
            pltpu.VMEM((grid, 2 * grid), BF16),
            pltpu.VMEM((mp, frames, grid), F32),
            pltpu.VMEM((frames, grid), F32),
            pltpu.VMEM((mp, quarter, grid), F32),
            pltpu.VMEM((group, mp, quarter, grid), F32),
            pltpu.VMEM((mp, quarter, grid), F32),
            pltpu.VMEM((frames, grid), F32),
            pltpu.VMEM((group, 8, grid), F32),
            pltpu.VMEM((8, grid), F32),
            pltpu.VMEM((8, grid), F32),
            pltpu.VMEM((8, grid), F32),
            pltpu.VMEM((share, grid), F32),
            pltpu.VMEM((share, grid), F32),
            pltpu.VMEM((share, grid), F32),
            pltpu.VMEM((2, grid), F32),
            pltpu.VMEM((tm * mp, 2, grid), F32),
            dma((8 + chunks,)),
            dma((mp,)), dma((mp,)),
            *[dma((group,))] * 8,
            dma((mp,)), dma((mp,)),
            dma((group,)), dma((group,)),
            dma(()), dma(()),
            dma((tm * mp,)), dma((tm * mp,)),
        ],
        compiler_params=pltpu.CompilerParams(
            collective_id=0, has_side_effects=True
        ),
        name="track",
    )(*args)
    whole = pl.BlockSpec(memory_space=pltpu.VMEM)
    return pl.pallas_call(
        functools.partial(finish, share),
        out_shape=(out, out),
        in_specs=[whole],
        out_specs=(whole, whole),
        name="finish",
    )(packed)


def solution(mesh):
    placed = (
        P("tm", None),
        P(None, "mp"),
        P("mp"),
        P("mp", None),
        P(),
        P(),
        P("tm", None),
        P("tm", None),
    )
    return jax.shard_map(
        on_device,
        mesh=mesh,
        in_specs=placed,
        out_specs=(P(("tm", "mp"), None), P(("tm", "mp"), None)),
        check_vma=False,
    )
```

```python
import functools
import math

import jax
import jax.numpy as jnp
from jax import lax
from jax.experimental import pallas as pl
from jax.experimental.pallas import tpu as pltpu
from jax.sharding import PartitionSpec as P

MESH = pl.DeviceIdType.MESH
F32 = jnp.float32
BF16 = jnp.bfloat16
GROUP = 4


def split(value):
    high = value.astype(BF16).astype(F32)
    return high, value - high


def store_split(target, value):
    width = value.shape[1]
    high, rest = split(value)
    target[:, :width] = high.astype(BF16)
    target[:, width:] = rest.astype(BF16)


def store_product(target, quarters):
    count, rows, grid = quarters.shape
    store_split(target, quarters[...].reshape(count * rows, grid))


def times(rows, pair):
    count, width = rows.shape
    both = jnp.concatenate(split(rows), 0).astype(BF16)
    out = jnp.dot(both, pair[...], preferred_element_type=F32)
    return out[:count, :width] + out[count:, :width] + out[:count, width:]


def kernel(
    tm, mp, chunks, group,
    feat_h, w_in_h, b_h, w2_h, off_h, trans_h, gains_h, sg_h,
    packed,
    feat, w_in, b_v, w2, off, trans, gains, sg,
    at, at_pair, m_pair, phi_pair, part, meas, snap, m_all, phi_all, vel, v_all, x_in, x_out, x_own,
    f8, u8, e8, slope_own, value_own, slopes, values, shares,
    in_sem, part_ss, part_rs, r1_ss, r1_rs, r2_ss, r2_rs, r3_ss, r3_rs, r4_ss, r4_rs,
    phi_ss, phi_rs, v_ss, v_rs, chain_ss, chain_rs, slope_ss, slope_rs, back_ss, back_rs,
):
    c, k = lax.axis_index("tm"), lax.axis_index("mp")
    place = c * mp + k
    total = tm * mp
    here, set_c = lax.rem(c, group), c // group
    sets = tm // group
    across = lax.rem(k + mp // 2, mp)
    beside = k + 1 - 2 * lax.rem(k, 2)
    frames, grid = gains.shape
    share = frames // mp
    quarter = grid // mp
    depth = feat.shape[1] // chunks

    def fetch(source, target, slot):
        copy = pltpu.make_async_copy(source, target, in_sem.at[slot])
        copy.start()
        return copy

    get_trans = fetch(trans_h, trans, 0)
    get_gains = fetch(gains_h, gains, 1)
    get_feat = fetch(feat_h, feat, 2)
    get_w = [
        fetch(w_in_h.at[pl.ds(r * depth, depth), :], w_in.at[pl.ds(r * depth, depth), :], 8 + r)
        for r in range(chunks)
    ]
    get_b = fetch(b_h, b_v, 3)
    get_w2 = fetch(w2_h, w2, 4)
    get_off = fetch(off_h, off, 5)
    get_sg = fetch(sg_h, sg, 6)

    barrier = pltpu.get_barrier_semaphore()

    def greet(step, carry):
        other = lax.rem(place + step, total)
        pl.semaphore_signal(
            barrier, inc=1, device_id={"tm": other // mp, "mp": lax.rem(other, mp)},
            device_id_type=MESH,
        )
        return carry

    lax.fori_loop(1, total, greet, 0)

    get_trans.wait()
    get_gains.wait()
    at[...] = jnp.transpose(trans[...])
    store_split(at_pair, at[...])
    rows = at[pl.ds(pl.multiple_of(k * quarter, quarter), quarter), :] * (1.0 - gains[0:1, :])
    get_feat.wait()
    pre = jnp.zeros((frames, w_in.shape[1]), F32)
    def advance(rows, first, end):
        for t in range(first, end):
            if t > 0:
                rows = times(rows, at_pair) * (1.0 - gains[t : t + 1, :])
            if (t + 1) % share == 0:
                snap[(t + 1) // share - 1] = rows
        return rows

    pace = frames // chunks // 2
    for r in range(chunks):
        get_w[r].wait()
        pre += jnp.dot(
            feat[:, r * depth : (r + 1) * depth], w_in[r * depth : (r + 1) * depth, :],
            preferred_element_type=F32,
        )
        rows = advance(rows, r * pace, (r + 1) * pace)
    get_b.wait()
    get_w2.wait()
    hidden = jax.nn.gelu(pre + b_v[...], approximate=True).astype(BF16)
    part[k] = jnp.dot(hidden, w2[...], preferred_element_type=F32)

    pl.semaphore_wait(barrier, total - 1)

    def remote(source, target, send, recv, c_to, k_to):
        return pltpu.make_async_remote_copy(
            source, target, send, recv, device_id={"tm": c_to, "mp": k_to}, device_id_type=MESH
        )

    def phi_copy(step):
        peer = lax.rem(k + step, mp)
        return remote(
            snap.at[lax.rem(peer + mp - 1, mp)], phi_all.at[k], phi_ss.at[step], phi_rs.at[step],
            c, peer,
        )

    def in_set(step, source, target, send, recv):
        peer = set_c * group + lax.rem(here + step, group)
        return remote(source, target, send.at[step], recv.at[step], peer, k)

    part_copies = [
        remote(part.at[k], part.at[k], part_ss.at[s], part_rs.at[s], c, lax.rem(k + s, mp))
        for s in range(1, mp)
    ]
    for copy in part_copies:
        copy.start()
    rows = advance(rows, pace * chunks, frames)

    own = snap.at[mp - 1]
    come = [lax.rem(here + group - s, group) for s in range(group)]
    r1 = [in_set(s, own, m_all.at[here, k], r1_ss, r1_rs) for s in range(1, group)]
    r2, r3, r4 = [], [], []
    for s in range(group):
        j = come[s]
        mine = own if s == 0 else m_all.at[j, k]
        r2.append(remote(mine, m_all.at[j, k], r2_ss.at[s], r2_rs.at[s], c, across))
        r3.append(remote(mine, m_all.at[j, k], r3_ss.at[s], r3_rs.at[s], c, beside))
        r4.append(
            remote(m_all.at[j, across], m_all.at[j, across], r4_ss.at[s], r4_rs.at[s], c, beside)
        )
    phi_copies = [phi_copy(s) for s in range(1, mp)]
    def need(reader, j):
        return ((j < reader) | (set_c < sets - 1)) & ((set_c > 0) | (j > 0))

    def when(condition, *actions):
        @pl.when(condition)
        def _():
            for action in actions:
                action()

    wanted = [need(here, come[s]) for s in range(group)]
    given = [need(lax.rem(here + s, group), here) for s in range(group)]
    for s in range(1, group):
        when(given[s], r1[s - 1].start)
    when(wanted[0], r2[0].start, r3[0].start)
    m_all[here, k] = snap[mp - 1]
    phi_all[k] = snap[lax.rem(k + mp - 1, mp)]
    get_off.wait()
    get_sg.wait()
    for copy in part_copies:
        copy.wait_recv()
    measured = off[...]
    for peer in range(mp):
        measured = measured + part[peer]
    meas[...] = gains[...] * measured

    def frame(t, state):
        keep = 1.0 - gains[pl.ds(t, 1), :]
        return times(state, at_pair) * keep + meas[pl.ds(t, 1), :]

    def pass_frames(block, state):
        for j in range(share):
            t = block * share + j
            state = frame(t, state)
            vel[pl.ds(t, 1), :] = state[0:1]
        return state

    early = 3 * mp // 4
    vel_end = lax.fori_loop(0, early, pass_frames, jnp.zeros((8, grid), F32))
    for s in range(1, group):
        when(wanted[s], r1[s - 1].wait_recv, r2[s].start, r3[s].start)
    for copy in phi_copies:
        copy.start()
    vel_end = lax.fori_loop(early, mp, pass_frames, vel_end)
    v_all[here] = vel_end
    v_copies = [in_set(s, v_all.at[here], v_all.at[here], v_ss, v_rs) for s in range(1, group)]
    for copy in v_copies:
        copy.start()
    last = jnp.where(place == total - 1, 0.0, 1.0).astype(F32)
    row = lax.broadcasted_iota(jnp.int32, (share, grid), 0)
    weight = sg[pl.ds(pl.multiple_of(k * share, share), share), :]
    e8[...] = jnp.where(row == share - 1, weight * last, weight)
    slope = e8[0:1, :]
    for j in range(1, share):
        slope = slope * e8[j : j + 1, :]
    slope_own[...] = slope

    def back_copy(own, target, send, recv, other):
        return remote(
            own, target.at[place], send.at[other], recv.at[place], other // mp, lax.rem(other, mp)
        )

    def from_later(own, target, send, recv, source):
        return remote(
            own, target.at[source], send.at[source], recv.at[source],
            source // mp, lax.rem(source, mp),
        )

    to_slopes = (slope_own, slopes, slope_ss, slope_rs)
    to_values = (value_own, values, back_ss, back_rs)

    def send_slope(other, carry):
        back_copy(*to_slopes, other).start()
        return carry

    def send_value(other, carry):
        back_copy(*to_values, other).start()
        return carry

    lax.fori_loop(0, place, send_slope, 0)
    for s in range(group):
        when(wanted[s], r2[s].wait_recv, r4[s].start)
    for s in range(group):
        when(
            wanted[s], r3[s].wait_recv, r4[s].wait_recv,
            functools.partial(store_product, m_pair.at[come[s]], m_all.at[come[s]]),
        )

    @pl.when(set_c == 0)
    def _():
        m_pair[0] = jnp.zeros_like(m_pair[0])

    for copy in v_copies:
        copy.wait_recv()

    chain = remote(x_out, x_in, chain_ss, chain_rs, lax.rem(c + group, tm), k)

    @pl.when(set_c == 0)
    def _():
        x_in[...] = jnp.zeros_like(x_in)

    keep_phi = functools.partial(store_product, phi_pair, phi_all)
    when(set_c > 0, *[copy.wait_recv for copy in phi_copies], keep_phi, chain.wait_recv)

    def whole_block(j, state):
        return times(state, m_pair.at[j]) + v_all[j]

    state = lax.fori_loop(0, here, whole_block, x_in[...])

    @pl.when(set_c < sets - 1)
    def _():
        x_out[...] = lax.fori_loop(here, group, whole_block, state)
        chain.start()

    x_in[...] = state
    when(set_c == 0, *[copy.wait_recv for copy in phi_copies], keep_phi)

    @pl.when(k == 0)
    def _():
        x_own[...] = x_in[...]

    @pl.when(k > 0)
    def _():
        x_own[...] = times(x_in[...], phi_pair) + vel[pl.ds(k * share - 1, 1), :]

    state = x_own[...]
    for j in range(share):
        state = frame(k * share + j, state)
        f8[j : j + 1, :] = state[0:1]
    filtered = f8[...]
    packed[:share, :] = filtered
    weight = e8[...]
    u8[...] = filtered - weight * times(filtered, at_pair)
    value = u8[share - 1 : share, :]
    for j in range(share - 2, -1, -1):
        value = u8[j : j + 1, :] + e8[j : j + 1, :] * value
    value_own[...] = value
    lax.fori_loop(0, place, send_value, 0)
    packed[share : 2 * share, :] = u8[...]
    packed[2 * share : 3 * share, :] = weight

    def weigh(source, part):
        from_later(*to_slopes, source).wait_recv()
        shares[source] = part
        return part * slopes[source]

    def add_up(source, later):
        from_later(*to_values, source).wait_recv()
        return later + shares[source] * values[source]

    lax.fori_loop(place + 1, total, weigh, jnp.ones((1, grid), F32))
    later = lax.fori_loop(place + 1, total, add_up, jnp.zeros((1, grid), F32))
    packed[3 * share :, :] = jnp.broadcast_to(later, (8, grid))

    def end_back(other, carry):
        back_copy(*to_slopes, other).wait_send()
        back_copy(*to_values, other).wait_send()
        return carry

    lax.fori_loop(0, place, end_back, 0)
    for copy in part_copies + v_copies + phi_copies:
        copy.wait_send()
    for s in range(group):
        if s > 0:
            when(given[s], r1[s - 1].wait_send)
        when(wanted[s], r2[s].wait_send, r3[s].wait_send, r4[s].wait_send)

    @pl.when(set_c < sets - 1)
    def _():
        chain.wait_send()


def finish(share, packed, filt_o, smooth_o):
    filt_o[...] = packed[:share, :]
    later = packed[3 * share : 3 * share + 1, :]
    for j in range(share - 1, -1, -1):
        fresh, weight = share + j, 2 * share + j
        later = packed[fresh : fresh + 1, :] + packed[weight : weight + 1, :] * later
        smooth_o[j : j + 1, :] = later


def on_device(features, w_in, b_in, output_weight, offset, transition, gains, smooth_gains):
    tm, mp = lax.axis_size("tm"), lax.axis_size("mp")
    frames, lags = features.shape
    units = w_in.shape[1]
    grid = transition.shape[0]
    share = frames // mp
    quarter = grid // mp
    chunks = 8
    group = math.gcd(tm, GROUP)
    args = (
        features, w_in, b_in.reshape(1, units), output_weight, offset.reshape(1, grid),
        transition, gains, smooth_gains,
    )
    dma = pltpu.SemaphoreType.DMA
    out = jax.ShapeDtypeStruct((share, grid), F32)
    packed = pl.pallas_call(
        functools.partial(kernel, tm, mp, chunks, group),
        out_shape=jax.ShapeDtypeStruct((3 * share + 8, grid), F32),
        in_specs=[pl.BlockSpec(memory_space=pl.ANY)] * len(args),
        out_specs=pl.BlockSpec(memory_space=pltpu.VMEM),
        scratch_shapes=[pltpu.VMEM(a.shape, a.dtype) for a in args]
        + [
            pltpu.VMEM((grid, grid), F32),
            pltpu.VMEM((grid, 2 * grid), BF16),
            pltpu.VMEM((group, grid, 2 * grid), BF16),
            pltpu.VMEM((grid, 2 * grid), BF16),
            pltpu.VMEM((mp, frames, grid), F32),
            pltpu.VMEM((frames, grid), F32),
            pltpu.VMEM((mp, quarter, grid), F32),
            pltpu.VMEM((group, mp, quarter, grid), F32),
            pltpu.VMEM((mp, quarter, grid), F32),
            pltpu.VMEM((frames, grid), F32),
            pltpu.VMEM((group, 8, grid), F32),
            pltpu.VMEM((8, grid), F32),
            pltpu.VMEM((8, grid), F32),
            pltpu.VMEM((8, grid), F32),
            pltpu.VMEM((share, grid), F32),
            pltpu.VMEM((share, grid), F32),
            pltpu.VMEM((share, grid), F32),
            pltpu.VMEM((1, grid), F32),
            pltpu.VMEM((1, grid), F32),
            pltpu.VMEM((tm * mp, 1, grid), F32),
            pltpu.VMEM((tm * mp, 1, grid), F32),
            pltpu.VMEM((tm * mp, 1, grid), F32),
            dma((8 + chunks,)),
            dma((mp,)), dma((mp,)),
            *[dma((group,))] * 8,
            dma((mp,)), dma((mp,)),
            dma((group,)), dma((group,)),
            dma(()), dma(()),
            *[dma((tm * mp,))] * 4,
        ],
        compiler_params=pltpu.CompilerParams(
            collective_id=0, has_side_effects=True
        ),
        name="track",
    )(*args)
    whole = pl.BlockSpec(memory_space=pltpu.VMEM)
    return pl.pallas_call(
        functools.partial(finish, share),
        out_shape=(out, out),
        in_specs=[whole],
        out_specs=(whole, whole),
        name="finish",
    )(packed)


def solution(mesh):
    placed = (
        P("tm", None),
        P(None, "mp"),
        P("mp"),
        P("mp", None),
        P(),
        P(),
        P("tm", None),
        P("tm", None),
    )
    return jax.shard_map(
        on_device,
        mesh=mesh,
        in_specs=placed,
        out_specs=(P(("tm", "mp"), None), P(("tm", "mp"), None)),
        check_vma=False,
    )
```
